32 devices in a mesh: ka: 2 (over x), band: 16 (over z, y, core).
Axes of the slice: x: 2, y: 2, z: 4, core: 2. Of those that a mesh axis runs over, the one named last changes fastest.
Arguments:
- psi_hat: float32 [2, 12, 2, 128, 128, 128], P('ka', None, None, 'band'), may hold values from -1.5 to 1.5
- occupations: int32 [2, 12], P('ka'), may hold values from 0 to 2
- weights: int32 [2], P('ka'), may hold values from 1 to 6
- density_in: float32 [128, 128, 128], P('band'), may hold values from -12 to 12
- dens_hist: float32 [8, 128, 128, 128], P(None, 'band'), may hold values from -3 to 3
- resid_hist: float32 [8, 128, 128, 128], P(None, 'band'), may hold values from -12 to 12
Outputs:
- out_density: float32 [128, 128, 128], P('band')
- mixed_density: float32 [128, 128, 128], P('band')
The draws below stay inside these ranges and needn't reach their ends.
All inputs are finite; a program needn't handle non-finite values.
Results may differ from the reference program's by a relative error of at most 0.0003.
Values sent between devices are 32-bit elements; how exact they have to be, the bound alone decides.
A program may use at most 128 MiB of HBM per device.

```python
from functools import partial
import jax
import jax.numpy as jnp
from jax import lax

NG = 128
BANDS = 12
HIST = 8
KPTS = 2


def common_field(key):
    return jax.random.truncated_normal(jax.random.fold_in(key, 7), -5.0, 5.0, (NG, NG, NG), jnp.float32)


def draw_density_in(key, part):
    shared = common_field(key)
    noise_part = jax.random.truncated_normal(jax.random.fold_in(key, 11), -5.0, 5.0, (NG, NG, NG), jnp.float32)
    return shared + 0.3 * noise_part


def draw_resid_hist(key, part):
    shared = common_field(key)
    loadings = jax.random.uniform(jax.random.fold_in(key, 13), (HIST, 1, 1, 1), jnp.float32, -1.0, 1.0)
    noise_part = jax.random.truncated_normal(jax.random.fold_in(key, 17), -5.0, 5.0, (HIST, NG, NG, NG), jnp.float32)
    return loadings * shared + 0.5 * noise_part


def touch_ends(array, stream_key, least, largest):
    longest = array.shape.index(max(array.shape))
    spots = []
    for shift in (0, 1):
        where = [jax.random.randint(jax.random.fold_in(stream_key, axis), (), 0, length) for axis, length in enumerate(array.shape)]
        where[longest] = (where[longest] + shift) % array.shape[longest]
        spots.append(tuple(where))
    return array.at[spots[0]].set(least).at[spots[1]].set(largest)


def level_of(stream_key, dims, split, smallest, top_value):
    level = 1.0
    for dim, parts in split:
        heights = jax.random.uniform(jax.random.fold_in(jax.random.fold_in(stream_key, 6), dim), (parts,), jnp.float32, smallest / len(split), top_value / len(split))
        level = level * jnp.repeat(jnp.exp(heights), dims[dim] // parts).reshape((-1,) + (1,) * (len(dims) - 1 - dim))
    return level


def gaussian(stream_key, shape, deviation, most, cuts=(), kind=jnp.bfloat16):
    gain = level_of(stream_key, shape, cuts, -0.22, 0.18) if cuts else 1.0
    result = jax.random.normal(stream_key, shape, jnp.float32) * deviation * gain
    return jnp.minimum(jnp.maximum(result, -most), most).astype(kind)


def setup_inputs(seed: int = 0) -> dict:
    key_list = jax.random.split(jax.random.key(seed), 7)
    psi_hat = gaussian(key_list[0], (KPTS, BANDS, 2, NG, NG, NG), 0.25, 1.5, ((0, 2), (3, 16)), jnp.float32)
    occupations = touch_ends(jax.random.randint(key_list[1], (KPTS, BANDS), 0, 3), jax.random.fold_in(key_list[1], 1), 0, 2).astype(jnp.int32)
    weights = jax.random.randint(key_list[2], (KPTS,), 1, 7).astype(jnp.int32)
    density_in = draw_density_in(jax.random.fold_in(key_list[6], 71), 0)
    dens_hist = gaussian(key_list[4], (HIST, NG, NG, NG), 0.5, 3.0, ((1, 16),), jnp.float32)
    resid_hist = draw_resid_hist(jax.random.fold_in(key_list[6], 71), 0)
    return dict(psi_hat=psi_hat, occupations=occupations, weights=weights, density_in=density_in, dens_hist=dens_hist, resid_hist=resid_hist)


highest = lax.Precision.HIGHEST
beta_mix = 0.3
regular = 0.01

def dft_tables():
    indices = jnp.arange(NG, dtype=jnp.int32)
    product = indices[:, None] * indices[None, :] % NG
    angles = product.astype(jnp.float32) * jnp.float32(2.0 * 3.141592653589793 / NG)
    return (jnp.cos(angles), jnp.sin(angles))

def rotate(pattern, real_part, imag_part, cosine_table, sine_table):
    einsum = partial(jnp.einsum, precision=highest)
    out_real = einsum(pattern, real_part, cosine_table) - einsum(pattern, imag_part, sine_table)
    out_imag = einsum(pattern, real_part, sine_table) + einsum(pattern, imag_part, cosine_table)
    return (out_real, out_imag)

def band_power(coeffs, cosine_table, sine_table):
    real_part, imag_part = rotate('pqk,kz->zpq', coeffs[0], coeffs[1], cosine_table, sine_table)
    real_part, imag_part = rotate('zpq,qy->zpy', real_part, imag_part, cosine_table, sine_table)
    real_part, imag_part = rotate('zpy,px->zxy', real_part, imag_part, cosine_table, sine_table)
    return (real_part * real_part + imag_part * imag_part) * jnp.float32(1.0 / NG ** 3)

def broyden(density, density_in, dens_hist, resid_hist):
    residual_now = density - density_in
    gram = jnp.einsum('hzxy,gzxy->hg', resid_hist, resid_hist, precision=highest)
    projections = jnp.einsum('hzxy,zxy->h', resid_hist, residual_now, precision=highest)
    system = gram + regular * jnp.diag(jnp.diag(gram))
    chol_factor = jnp.linalg.cholesky(system)
    mix_coefs = jax.scipy.linalg.cho_solve((chol_factor, True), projections)
    update = jnp.einsum('h,hzxy->zxy', mix_coefs, dens_hist + beta_mix * resid_hist, precision=highest)
    return density_in + beta_mix * residual_now - update

def reference(psi_hat, occupations, weights, density_in, dens_hist, resid_hist):
    cosine_table, sine_table = dft_tables()
    weight_total = jnp.sum(weights.astype(jnp.float32))

    def per_point(point_total, point_inputs):
        coeffs_point, occ_point, weight_point = point_inputs

        def per_band(band_total, band_inputs):
            coeffs_band, occ_band = band_inputs
            power = band_power(coeffs_band, cosine_table, sine_table)
            return (band_total + occ_band.astype(jnp.float32) * power, None)
        pool_term, unused = lax.scan(per_band, jnp.zeros((NG, NG, NG), jnp.float32), (coeffs_point, occ_point))
        return (point_total + pool_term * (weight_point.astype(jnp.float32) / weight_total), None)
    density, unused = lax.scan(per_point, jnp.zeros((NG, NG, NG), jnp.float32), (psi_hat, occupations, weights))
    mixed_density = broyden(density, density_in, dens_hist, resid_hist)
    return (density, mixed_density)
```

```python
from functools import partial

import jax
import jax.numpy as jnp
import numpy as np
from jax import lax
from jax.experimental import pallas as pl
from jax.experimental.pallas import tpu as pltpu
from jax.sharding import PartitionSpec as P

highest = lax.Precision.HIGHEST
beta_mix = 0.3
regular = 0.01
CHUNKS = 3


def rotation_tables(size):
    indices = np.arange(size)
    angles = (indices[:, None] * indices[None, :] % size) * (2.0 * np.pi / size)
    cosine, sine = np.cos(angles), np.sin(angles)
    table = np.block([[cosine, sine], [-sine, cosine]]).astype(np.float32)
    high = table.astype(jnp.bfloat16)
    low = (table - high.astype(np.float32)).astype(jnp.bfloat16)
    return high, low


def split(value):
    high = value.astype(jnp.bfloat16)
    return high, (value - high.astype(jnp.float32)).astype(jnp.bfloat16)


def dot3(left, right, contract):
    dims = (contract, ((), ()))
    dot = partial(lax.dot_general, dimension_numbers=dims, preferred_element_type=jnp.float32)
    return dot(left[0], right[0]) + (dot(left[0], right[1]) + dot(left[1], right[0]))


def planes_kernel(psi_ref, wh_ref, wl_ref, th_ref, tl_ref, out_ref):
    devices, _, _, depth, planes, size = out_ref.shape
    for p in range(planes):
        pair = jnp.concatenate([psi_ref[0, 0, 0, p], psi_ref[0, 0, 1, p]], axis=1)
        after_kz = dot3((th_ref[...], tl_ref[...]), split(pair), ((1,), (1,)))
        rows = jnp.concatenate([after_kz[:size], after_kz[size:]], axis=1)
        after_ky = dot3(split(rows), (wh_ref[...], wl_ref[...]), ((1,), (0,)))
        for part in range(2):
            piece = after_ky[:, part * size : (part + 1) * size]
            out_ref[:, 0, part, :, p, :] = piece.reshape(devices, depth, size)


def power_kernel(scale_ref, recv_ref, th_ref, tl_ref, prev_ref, out_ref):
    devices, _, _, depth, planes, size = recv_ref.shape
    band = pl.program_id(0)
    factor = scale_ref[band]

    @pl.when(band == 0)
    def _():
        out_ref[...] = prev_ref[...]

    for z in range(0, depth, 2):
        columns = []
        for near in range(2):
            parts = [recv_ref[:, 0, c, z + near].reshape(devices * planes, size) for c in range(2)]
            columns.append(jnp.concatenate(parts, axis=0))
        field = dot3(
            (th_ref[...], tl_ref[...]), split(jnp.concatenate(columns, axis=1)), ((1,), (0,))
        )
        power = field[:size] * field[:size] + field[size:] * field[size:]
        for near in range(2):
            out_ref[z + near] += factor * power[:, near * size : (near + 1) * size]


def shards(psi_hat, occupations, weights, density_in, dens_hist, resid_hist):
    devices, points = lax.axis_size("band"), lax.axis_size("ka")
    _, bands, _, planes, size, _ = psi_hat.shape
    depth = size // devices
    chunks = CHUNKS if bands % CHUNKS == 0 else 1
    count = bands // chunks
    high, low = rotation_tables(size)
    wh, wl, th, tl = (jnp.asarray(t) for t in (high, low, high.T, low.T))

    weight = weights[0].astype(jnp.float32)
    share = weight / lax.psum(weight, "ka")
    factors = occupations[0].astype(jnp.float32) * (share * jnp.float32(1.0 / size**3))

    flops = 3 * 2 * count * planes * size * (2 * size) ** 2
    bytes_each = count * 2 * planes * size * size * 4
    whole = pl.BlockSpec((2 * size, 2 * size), lambda b: (0, 0))
    tile_spec = pl.BlockSpec((devices, 1, 2, depth, planes, size), lambda b: (0, b, 0, 0, 0, 0))
    slab = pl.BlockSpec((depth, size, size), lambda b: (0, 0, 0))
    limit = 40 * 1024 * 1024

    received = []
    for chunk in range(chunks):
        tiles = pl.pallas_call(
            planes_kernel,
            grid=(count,),
            in_specs=[
                pl.BlockSpec(
                    (1, 1, 2, planes, size, size),
                    lambda b, first=chunk * count: (0, first + b, 0, 0, 0, 0),
                ),
                whole, whole, whole, whole,
            ],
            out_specs=tile_spec,
            out_shape=jax.ShapeDtypeStruct(
                (devices, count, 2, depth, planes, size), jnp.float32
            ),
            compiler_params=pltpu.CompilerParams(vmem_limit_bytes=limit),
            cost_estimate=pl.CostEstimate(
                flops=2 * flops, bytes_accessed=2 * bytes_each, transcendentals=0
            ),
        )(psi_hat, wh, wl, th, tl)
        received.append(lax.all_to_all(tiles, "band", split_axis=0, concat_axis=0, tiled=True))

    gram = jnp.einsum("hzxy,gzxy->hg", resid_hist, resid_hist, precision=highest)
    start = jnp.einsum("hzxy,zxy->h", resid_hist, density_in, precision=highest)
    early = lax.psum(jnp.concatenate([gram, start[:, None]], axis=1), ("ka", "band"))
    early = early * jnp.float32(1.0 / points)
    gram, start = early[:, :-1], early[:, -1]
    system = gram + regular * jnp.diag(jnp.diag(gram))
    chol_factor = jnp.linalg.cholesky(system)

    pool = jnp.zeros((depth, size, size), jnp.float32)
    for chunk in range(chunks):
        pool = pl.pallas_call(
            power_kernel,
            grid=(count,),
            in_specs=[
                pl.BlockSpec(memory_space=pltpu.SMEM), tile_spec, whole, whole, slab,
            ],
            out_specs=slab,
            out_shape=jax.ShapeDtypeStruct((depth, size, size), jnp.float32),
            compiler_params=pltpu.CompilerParams(vmem_limit_bytes=limit),
            cost_estimate=pl.CostEstimate(
                flops=flops, bytes_accessed=bytes_each, transcendentals=0
            ),
        )(factors[chunk * count : (chunk + 1) * count], received[chunk], th, tl, pool)

    if points == 2:
        density = pool + lax.ppermute(pool, "ka", [(0, 1), (1, 0)])
    else:
        density = lax.psum(pool, "ka")
    late = lax.psum(jnp.sum(resid_hist * pool, axis=(1, 2, 3)), ("ka", "band"))
    mix_coefs = jax.scipy.linalg.cho_solve((chol_factor, True), late - start)
    history = dens_hist + beta_mix * resid_hist
    update = jnp.sum(mix_coefs[:, None, None, None] * history, axis=0)
    mixed_density = density_in + beta_mix * (density - density_in) - update
    return (density, mixed_density)


def solution(mesh):
    return jax.shard_map(
        shards,
        mesh=mesh,
        in_specs=(
            P("ka", None, None, "band", None, None),
            P("ka", None),
            P("ka"),
            P("band", None, None),
            P(None, "band", None, None),
            P(None, "band", None, None),
        ),
        out_specs=(P("band", None, None), P("band", None, None)),
        check_vma=False,
    )
```
